256 devices in a mesh: ord: 16 (over x, z_hi, core), blk: 16 (over z_lo, y).
Axes of the slice: x: 4, y: 4, z: 8 (z_hi: 2, z_lo: 4; z = z_hi * 4 + z_lo), core: 2. Of those that a mesh axis runs over, the one named last changes fastest.
Arguments:
- coefficients: bfloat16 [128, 2, 256, 8192], P('ord', None, None, 'blk'), may hold values from -0.52734375 to 0.52734375
- leaf_factors: bfloat16 [128, 128, 8192], P('ord', None, 'blk'), may hold values from -0.25 to 0.25
- level_interpolants: bfloat16 [3, 2, 128, 128, 2048], P(None, None, 'ord', None, 'blk'), may hold values from -0.375 to 0.375
- latitude_factors: bfloat16 [128, 10240, 128], P('ord', 'blk'), may hold values from -0.5 to 0.5
- order_ids: int32 [128], replicated, may hold values from 0 to 8191, as said below
Outputs:
- products: bfloat16 [256, 128, 10240], P(None, 'ord', 'blk')
The draws below stay inside these ranges and needn't reach their ends.
Inputs may be any that keep to these rules, and one draw needn't show every extreme that they name: `order_ids`: the slots hold distinct orders of the truncation.
All inputs are finite; a program needn't handle non-finite values.
Results may differ from the reference program's by a relative error of at most 0.011.
Values may be sent and summed in bfloat16 or wider, within the bound.
No kernel may reach another device: no remote copies, remote signals or barrier semaphores. Data moves between devices by JAX's collectives and lax.ppermute only.
A program may use at most 64 MiB of HBM per device.

```python
import math
import jax
import jax.numpy as jnp
import numpy as np
from jax import lax

FIELDS = 256
LEAF = 512
RANK = 128
PERIOD = 16384
ORDER_RANGE = 8192
NLON = 256
LEVELS = 3
LAT_DEV = 640
ORDERS = 128
DEGREES = 8192
LATS = 10240
BLK_RANKS = 2048
PAIRS = 128
N_BLK = 16


def draw_order_ids(key, part):
    selected_block = jax.random.permutation(jax.random.fold_in(key, 7), ORDER_RANGE)
    return selected_block[:ORDERS].astype(jnp.int32)


def shard_levels(rng, shape, split, smallest, largest):
    level = 1.0
    for position, blocks in split:
        draws = jax.random.uniform(jax.random.fold_in(jax.random.fold_in(rng, 6), position), (blocks,), jnp.float32, smallest / len(split), largest / len(split))
        level = level * jnp.repeat(jnp.exp(draws), shape[position] // blocks).reshape((-1,) + (1,) * (len(shape) - 1 - position))
    return level


def scatter_about(rng, extent, deviation, bound, split=(), kind=jnp.bfloat16):
    values = jax.random.normal(rng, extent, jnp.float32) * deviation
    if len(split) > 0:
        values = shard_levels(rng, extent, split, -0.22, 0.18) * values
    return jnp.clip(values, min=-bound, max=bound).astype(kind)


def setup_inputs(seed: int = 0) -> dict:
    key_list = jax.random.split(jax.random.key(seed), 6)
    coefficients = scatter_about(key_list[0], (ORDERS, 2, FIELDS, DEGREES), (0.5 * ORDERS ** -0.5), 0.52734375, ((0, 16), (3, 16)))
    leaf_factors = scatter_about(key_list[1], (ORDERS, RANK, DEGREES), LEAF ** -0.5, 0.25, ((0, 16), (2, 16)))
    level_interpolants = scatter_about(key_list[2], (LEVELS, 2, ORDERS, RANK, BLK_RANKS), (2 * RANK) ** -0.5, 0.375, ((2, 16), (4, 16)))
    latitude_factors = scatter_about(key_list[3], (ORDERS, LATS, RANK), RANK ** -0.5, 0.5, ((0, 16), (1, 16)))
    order_ids = draw_order_ids(jax.random.fold_in(key_list[5], 71), 0)
    return {"coefficients": coefficients, "leaf_factors": leaf_factors, "level_interpolants": level_interpolants, "latitude_factors": latitude_factors, "order_ids": order_ids}


def synthesis_table(order_ids, count, period):
    steps = jnp.arange(count, dtype=jnp.int32)
    phase = ((order_ids[:, None].astype(jnp.int32) * steps[None, :]) % period).astype(jnp.float32) * (2.0 * math.pi / period)
    weight = jnp.where(order_ids == 0, 1.0, 2.0).astype(jnp.float32)[:, None]
    table = jnp.stack([weight * jnp.cos(phase), -weight * jnp.sin(phase)], axis=1)
    return table.astype(jnp.bfloat16)


def reference(coefficients, leaf_factors, level_interpolants, latitude_factors, order_ids):
    partner_lists = [np.arange(N_BLK) ^ (N_BLK >> (k + 1)) for k in range(LEVELS)]

    def per_order(items):
        coef, leafm, levm = items
        flat = coef.astype(jnp.float32).reshape(2 * FIELDS, N_BLK, LEAF)
        leaves = leafm.astype(jnp.float32).reshape(RANK, N_BLK, LEAF)
        combined_sum = jnp.einsum('cjl,rjl->cjr', flat, leaves).astype(jnp.bfloat16)
        levels = levm.astype(jnp.float32).reshape(LEVELS, 2, RANK, N_BLK, RANK)
        for k in range(LEVELS):
            partner_block = combined_sum[:, partner_lists[k], :]
            mixed = jnp.einsum('cjr,sjr->cjs', combined_sum.astype(jnp.float32), levels[k, 0])
            mixed = mixed + jnp.einsum('cjr,sjr->cjs', partner_block.astype(jnp.float32), levels[k, 1])
            combined_sum = mixed.astype(jnp.bfloat16)
        return combined_sum

    combined_sum = lax.map(per_order, (coefficients, leaf_factors, jnp.moveaxis(level_interpolants, 2, 0)))
    table = synthesis_table(order_ids, NLON, PERIOD).astype(jnp.float32)
    by_block = jnp.moveaxis(combined_sum, 2, 0)
    lat_blocks = jnp.moveaxis(latitude_factors.reshape(ORDERS, N_BLK, LAT_DEV, RANK), 1, 0)

    def per_block(items):
        red, lat = items
        values = jnp.einsum('mcr,mlr->mcl', red.astype(jnp.float32), lat.astype(jnp.float32))
        values = values.astype(jnp.bfloat16).reshape(ORDERS, 2, FIELDS, LAT_DEV)
        grid = jnp.einsum('mrk,mrfl->kfl', table, values.astype(jnp.float32))
        grid = grid.reshape(NLON, PAIRS, 2, LAT_DEV)
        return (grid[:, :, 0, :] * grid[:, :, 1, :]).astype(jnp.bfloat16)

    block_list = lax.map(per_block, (by_block, lat_blocks))
    return jnp.transpose(block_list, (1, 2, 0, 3)).reshape(NLON, PAIRS, LATS)
```

```python
import math

import jax
import jax.numpy as jnp
from jax import lax
from jax.sharding import PartitionSpec as P


PERIOD = 16384
NLON = 256
SPLIT = 384
PIECE = 128


def xor_permute(shard, axis, mask):
    return lax.ppermute(shard, axis, [(i, i ^ mask) for i in range(lax.axis_size(axis))])


def synthesis_table(order_ids, count, period):
    steps = jnp.arange(count, dtype=jnp.int32)
    phase = (order_ids[:, None] * steps[None, :] % period).astype(jnp.float32) * (
        2.0 * math.pi / period
    )
    weight = jnp.where(order_ids == 0, 1.0, 2.0).astype(jnp.float32)[:, None]
    table = jnp.stack([weight * jnp.cos(phase), -weight * jnp.sin(phase)], axis=1)
    return table.astype(jnp.bfloat16)


def per_device(coefficients, leaf_factors, level_interpolants, latitude_factors, order_ids):
    m, parts, fields, leaf = coefficients.shape
    size = lax.axis_size("ord")
    group = fields // size
    half = size // 2
    side = (lax.axis_index("ord") >> 1) & 1
    by_side = coefficients.reshape(m, parts, size // 4, 2, 2 * group, leaf)

    def leaves(which):
        chosen = lax.dynamic_index_in_dim(by_side, which, 3, keepdims=False)
        flat = chosen.reshape(m, parts * half * group, leaf)
        return jnp.einsum(
            "mcl,mrl->mcr", flat, leaf_factors, preferred_element_type=jnp.float32
        ).astype(jnp.bfloat16)

    top = lax.axis_size("blk") // 2

    def level(k, here, there):
        mixed = jnp.einsum(
            "mcx,mhx->mch", here, level_interpolants[k, 0], preferred_element_type=jnp.float32
        ) + jnp.einsum(
            "mcx,mhx->mch", there, level_interpolants[k, 1], preferred_element_type=jnp.float32
        )
        return mixed.astype(jnp.bfloat16)

    near, far = leaves(side), leaves(1 - side)
    crossing = lambda shard: xor_permute(shard, "ord", 2)
    pieces = [
        crossing(latitude_factors[:, i : i + PIECE])
        for i in range(0, latitude_factors.shape[1], PIECE)
    ]
    lat_far = (
        jnp.concatenate(pieces[: SPLIT // PIECE], 1),
        jnp.concatenate(pieces[SPLIT // PIECE :], 1),
    )
    for k in range(level_interpolants.shape[0]):
        near = level(k, near, xor_permute(near, "blk", top >> k))
        far = level(k, far, xor_permute(far, "blk", top >> k))
    crossed = crossing(far)
    groups = [[i for i in range(size) if (i >> 1) & 1 == s] for s in (0, 1)]

    def regroup(reduced, factors):
        values = jnp.einsum(
            "mcr,mlr->mcl", reduced, factors, preferred_element_type=jnp.float32
        ).astype(jnp.bfloat16)
        values = values.reshape(m * parts, half, group, -1)
        values = values.transpose(1, 2, 0, 3)
        return lax.all_to_all(values, "ord", 0, 0, axis_index_groups=groups, tiled=True)

    table = synthesis_table(order_ids, NLON, PERIOD).reshape(size // 4, 2, 2 * m * parts, NLON)

    def rows(which):
        return lax.dynamic_index_in_dim(table, which, 1, keepdims=False).reshape(half, m * parts, NLON)

    def partial_grid(which, values):
        return jnp.einsum("sak,sfal->kfl", rows(which), values, preferred_element_type=jnp.float32)

    base = partial_grid(side, regroup(near, latitude_factors))
    bases = (base[:, :, :SPLIT], base[:, :, SPLIT:])
    outs = []
    for part, factors in zip(bases, lat_far):
        grid = part + partial_grid(1 - side, regroup(crossed, factors))
        grid = grid.reshape(NLON, group // 2, 2, -1)
        outs.append((grid[:, :, 0, :] * grid[:, :, 1, :]).astype(jnp.bfloat16))
    return jnp.concatenate(outs, -1)


def solution(mesh):
    in_specs = (
        P("ord", None, None, "blk"),
        P("ord", None, "blk"),
        P(None, None, "ord", None, "blk"),
        P("ord", "blk", None),
        P(),
    )
    out_specs = P(None, "ord", "blk")

    return jax.shard_map(
        per_device, mesh=mesh, in_specs=in_specs, out_specs=out_specs, check_vma=False
    )
```

```python
import math

import jax
import jax.numpy as jnp
from jax import lax
from jax.experimental import pallas as pl
from jax.experimental.pallas import tpu as pltpu
from jax.sharding import PartitionSpec as P


PERIOD = 16384
NLON = 256
SPLIT = 384
PIECE = 128


def xor_permute(shard, axis, mask):
    return lax.ppermute(shard, axis, [(i, i ^ mask) for i in range(lax.axis_size(axis))])


def synthesis_table(order_ids, count, period):
    steps = jnp.arange(count, dtype=jnp.int32)
    phase = (order_ids[:, None] * steps[None, :] % period).astype(jnp.float32) * (
        2.0 * math.pi / period
    )
    weight = jnp.where(order_ids == 0, 1.0, 2.0).astype(jnp.float32)[:, None]
    table = jnp.stack([weight * jnp.cos(phase), -weight * jnp.sin(phase)], axis=1)
    return table.astype(jnp.bfloat16)


def latitude_values(reduced, factors, parts):
    m, count, rank = reduced.shape
    cols = count // parts
    lats = sum(f.shape[1] for f in factors)
    steps = lats // PIECE
    per = steps // len(factors)

    def body(reduced_ref, *refs):
        factor_refs, out_ref, wide = refs[: len(factors)], refs[-2], refs[-1]
        for j, factor_ref in enumerate(factor_refs):
            for i in range(per):
                for o in range(m):
                    acc = lax.dot_general(
                        reduced_ref[o],
                        factor_ref[o, i * PIECE : (i + 1) * PIECE],
                        (((1,), (1,)), ((), ())),
                        preferred_element_type=jnp.float32,
                    )
                    for p in range(parts):
                        wide[pl.ds(o * parts + p, cols, stride=m * parts), :] = acc[
                            p * cols : (p + 1) * cols
                        ]
                start = (j * per + i) * PIECE
                out_ref[:, :, start : start + PIECE] = (
                    wide[...].reshape(cols, m * parts, PIECE).astype(jnp.bfloat16)
                )

    flops = 2 * m * count * rank * lats
    return pl.pallas_call(
        body,
        out_shape=jax.ShapeDtypeStruct((cols, m * parts, lats), jnp.bfloat16),
        in_specs=[pl.BlockSpec(memory_space=pltpu.VMEM)] * (1 + len(factors)),
        out_specs=pl.BlockSpec(memory_space=pltpu.VMEM),
        scratch_shapes=[pltpu.VMEM((cols * m * parts, PIECE), jnp.float32)],
        compiler_params=pltpu.CompilerParams(vmem_limit_bytes=32 << 20),
        cost_estimate=pl.CostEstimate(flops=flops, bytes_accessed=2 * cols * m * parts * lats, transcendentals=0),
        name="latitude_values",
    )(reduced, *factors)


def field_products(table, near_values, far_values, first, out):
    half, group, mp, lats = near_values.shape
    nlon, depth = table.shape
    steps = far_values.shape[-1] // PIECE
    pairs = group // 2

    def body(table_ref, near_ref, far_ref, *refs):
        out_ref, wide = refs[-2], refs[-1]
        for p in range(pairs):
            sides = [
                jnp.concatenate(
                    [ref[:, f].reshape(half * mp, PIECE) for ref in (near_ref, far_ref)], 0
                )
                for f in (2 * p, 2 * p + 1)
            ]
            grid = jnp.dot(
                table_ref[...], jnp.concatenate(sides, 1), preferred_element_type=jnp.float32
            )
            wide[pl.ds(p, nlon, stride=pairs), :] = grid[:, :PIECE] * grid[:, PIECE:]
        out_ref[...] = wide[...].reshape(nlon, pairs, PIECE).astype(jnp.bfloat16)

    block = (half, group, mp, PIECE)
    in_specs = [
        pl.BlockSpec((nlon, depth), lambda i: (0, 0)),
        pl.BlockSpec(block, lambda i: (0, 0, 0, first + i)),
        pl.BlockSpec(block, lambda i: (0, 0, 0, i)),
    ]
    args, aliases = [table, near_values, far_values], {}
    if out is not None:
        in_specs.append(pl.BlockSpec(memory_space=pl.ANY))
        args.append(out)
        aliases = {3: 0}
    return pl.pallas_call(
        body,
        grid=(steps,),
        out_shape=jax.ShapeDtypeStruct((nlon, pairs, lats), jnp.bfloat16),
        in_specs=in_specs,
        out_specs=pl.BlockSpec((nlon, pairs, PIECE), lambda i: (0, 0, first + i)),
        scratch_shapes=[pltpu.VMEM((nlon * pairs, PIECE), jnp.float32)],
        input_output_aliases=aliases,
        compiler_params=pltpu.CompilerParams(vmem_limit_bytes=32 << 20),
        cost_estimate=pl.CostEstimate(
            flops=2 * nlon * depth * group * PIECE * steps,
            bytes_accessed=6 * nlon * pairs * PIECE * steps,
            transcendentals=0,
        ),
        name="field_products",
    )(*args)


def per_device(coefficients, leaf_factors, level_interpolants, latitude_factors, order_ids):
    m, parts, fields, leaf = coefficients.shape
    size = lax.axis_size("ord")
    group = fields // size
    half = size // 2
    side = (lax.axis_index("ord") >> 1) & 1
    by_side = coefficients.reshape(m, parts, size // 4, 2, 2 * group, leaf)

    def leaves(which):
        chosen = lax.dynamic_index_in_dim(by_side, which, 3, keepdims=False)
        flat = chosen.reshape(m, parts * half * group, leaf)
        return jnp.einsum(
            "mcl,mrl->mcr", flat, leaf_factors, preferred_element_type=jnp.float32
        ).astype(jnp.bfloat16)

    top = lax.axis_size("blk") // 2

    def level(k, here, there):
        mixed = jnp.einsum(
            "mcx,mhx->mch", here, level_interpolants[k, 0], preferred_element_type=jnp.float32
        ) + jnp.einsum(
            "mcx,mhx->mch", there, level_interpolants[k, 1], preferred_element_type=jnp.float32
        )
        return mixed.astype(jnp.bfloat16)

    near, far = leaves(side), leaves(1 - side)
    crossing = lambda shard: xor_permute(shard, "ord", 2)
    pieces = [crossing(latitude_factors[:, :SPLIT]), crossing(latitude_factors[:, SPLIT:])]
    for k in range(level_interpolants.shape[0]):
        near = level(k, near, xor_permute(near, "blk", top >> k))
        far = level(k, far, xor_permute(far, "blk", top >> k))
    crossed = crossing(far)
    groups = [[i for i in range(size) if (i >> 1) & 1 == s] for s in (0, 1)]

    def regroup(reduced, factors):
        values = latitude_values(reduced, factors, parts)
        values = values.reshape((half, group) + values.shape[1:])
        return lax.all_to_all(values, "ord", 0, 0, axis_index_groups=groups, tiled=True)

    table = synthesis_table(order_ids, NLON, PERIOD).reshape(size // 4, 2, 2 * m * parts, NLON)

    def rows(which):
        return lax.dynamic_index_in_dim(table, which, 1, keepdims=False).reshape(half * m * parts, NLON)

    both = jnp.concatenate([rows(side), rows(1 - side)], 0).T
    near_values = regroup(near, [latitude_factors])
    first = regroup(crossed, pieces[:1])
    second = regroup(crossed, pieces[1:])
    out = field_products(both, near_values, first, 0, None)
    return field_products(both, near_values, second, SPLIT // PIECE, out)


def solution(mesh):
    in_specs = (
        P("ord", None, None, "blk"),
        P("ord", None, "blk"),
        P(None, None, "ord", None, "blk"),
        P("ord", "blk", None),
        P(),
    )
    out_specs = P(None, "ord", "blk")

    return jax.shard_map(per_device, mesh=mesh, in_specs=in_specs, out_specs=out_specs, check_vma=False)
```

```python
import math

import jax
import jax.numpy as jnp
from jax import lax
from jax.experimental import pallas as pl
from jax.experimental.pallas import tpu as pltpu
from jax.sharding import PartitionSpec as P


PERIOD = 16384
NLON = 256
CUTS = (0, 384, 640)
PIECE = 128


def xor_permute(shard, axis, mask):
    return lax.ppermute(shard, axis, [(i, i ^ mask) for i in range(lax.axis_size(axis))])


def synthesis_table(order_ids, count, period):
    steps = jnp.arange(count, dtype=jnp.int32)
    phase = (order_ids[:, None] * steps[None, :] % period).astype(jnp.float32) * (
        2.0 * math.pi / period
    )
    weight = jnp.where(order_ids == 0, 1.0, 2.0).astype(jnp.float32)[:, None]
    table = jnp.stack([weight * jnp.cos(phase), -weight * jnp.sin(phase)], axis=1)
    return table.astype(jnp.bfloat16)


def latitude_values(reduced, factors, parts):
    m, count, rank = reduced.shape
    cols = count // parts
    lats = sum(f.shape[1] for f in factors)
    steps = lats // PIECE
    per = steps // len(factors)

    def body(reduced_ref, *refs):
        factor_refs, out_ref, wide = refs[: len(factors)], refs[-2], refs[-1]
        for j, factor_ref in enumerate(factor_refs):
            for i in range(per):
                for o in range(m):
                    acc = lax.dot_general(
                        reduced_ref[o],
                        factor_ref[o, i * PIECE : (i + 1) * PIECE],
                        (((1,), (1,)), ((), ())),
                        preferred_element_type=jnp.float32,
                    )
                    for p in range(parts):
                        wide[pl.ds(o * parts + p, cols, stride=m * parts), :] = acc[
                            p * cols : (p + 1) * cols
                        ]
                start = (j * per + i) * PIECE
                out_ref[:, :, start : start + PIECE] = (
                    wide[...].reshape(cols, m * parts, PIECE).astype(jnp.bfloat16)
                )

    flops = 2 * m * count * rank * lats
    return pl.pallas_call(
        body,
        out_shape=jax.ShapeDtypeStruct((cols, m * parts, lats), jnp.bfloat16),
        in_specs=[pl.BlockSpec(memory_space=pltpu.VMEM)] * (1 + len(factors)),
        out_specs=pl.BlockSpec(memory_space=pltpu.VMEM),
        scratch_shapes=[pltpu.VMEM((cols * m * parts, PIECE), jnp.float32)],
        compiler_params=pltpu.CompilerParams(vmem_limit_bytes=32 << 20),
        cost_estimate=pl.CostEstimate(flops=flops, bytes_accessed=2 * cols * m * parts * lats, transcendentals=0),
        name="latitude_values",
    )(reduced, *factors)


def split_values(reduced, factors, parts, group, order):
    m, count, rank = reduced.shape
    cols = count // parts
    dests = cols // group
    lats = factors.shape[1]
    mp = m * parts

    def body(order_ref, reduced_ref, factor_ref, *refs):
        outs, wide = refs[:-1], refs[-1]
        for start in range(0, lats, PIECE):
            for o in range(m):
                acc = lax.dot_general(
                    reduced_ref[o],
                    factor_ref[o, start : start + PIECE],
                    (((1,), (1,)), ((), ())),
                    preferred_element_type=jnp.float32,
                )
                for p in range(parts):
                    wide[pl.ds(o * parts + p, cols, stride=mp), :] = acc[p * cols : (p + 1) * cols]
            for k, out_ref in enumerate(outs):
                row = pl.multiple_of(order_ref[k] * (group * mp), group * mp)
                chosen = wide[pl.ds(row, group * mp), :]
                out_ref[:, :, start : start + PIECE] = chosen.reshape(group, mp, PIECE).astype(
                    jnp.bfloat16
                )

    return list(pl.pallas_call(
        body,
        out_shape=[jax.ShapeDtypeStruct((group, mp, lats), jnp.bfloat16)] * dests,
        in_specs=[pl.BlockSpec(memory_space=pltpu.SMEM)]
        + [pl.BlockSpec(memory_space=pltpu.VMEM)] * 2,
        out_specs=[pl.BlockSpec(memory_space=pltpu.VMEM)] * dests,
        scratch_shapes=[pltpu.VMEM((cols * mp, PIECE), jnp.float32)],
        compiler_params=pltpu.CompilerParams(vmem_limit_bytes=32 << 20),
        cost_estimate=pl.CostEstimate(
            flops=2 * m * count * rank * lats, bytes_accessed=2 * cols * mp * lats, transcendentals=0
        ),
        name="split_values",
    )(order, reduced, factors))


def field_products(table, near_values, far_values, first, out):
    half, group, mp, lats = near_values.shape
    nlon, depth = table.shape
    count = len(far_values)
    steps = far_values[0].shape[-1] // PIECE
    pairs = group // 2

    def body(table_ref, near_ref, *refs):
        far_refs, out_ref, wide = refs[:count], refs[-2], refs[-1]
        for p in range(pairs):
            sides = [
                jnp.concatenate(
                    [ref[:, f].reshape(-1, PIECE) for ref in (near_ref, *far_refs)], 0
                )
                for f in (2 * p, 2 * p + 1)
            ]
            grid = jnp.dot(
                table_ref[...], jnp.concatenate(sides, 1), preferred_element_type=jnp.float32
            )
            wide[pl.ds(p, nlon, stride=pairs), :] = grid[:, :PIECE] * grid[:, PIECE:]
        out_ref[...] = wide[...].reshape(nlon, pairs, PIECE).astype(jnp.bfloat16)

    block = (half, group, mp, PIECE)
    in_specs = [
        pl.BlockSpec((nlon, depth), lambda i: (0, 0)),
        pl.BlockSpec(block, lambda i: (0, 0, 0, first + i)),
    ]
    in_specs += [
        pl.BlockSpec((half // count, group, mp, PIECE), lambda i: (0, 0, 0, i)) for _ in range(count)
    ]
    args, aliases = [table, near_values, *far_values], {}
    if out is not None:
        in_specs.append(pl.BlockSpec(memory_space=pl.ANY))
        args.append(out)
        aliases = {2 + count: 0}
    return pl.pallas_call(
        body,
        grid=(steps,),
        out_shape=jax.ShapeDtypeStruct((nlon, pairs, lats), jnp.bfloat16),
        in_specs=in_specs,
        out_specs=pl.BlockSpec((nlon, pairs, PIECE), lambda i: (0, 0, first + i)),
        scratch_shapes=[pltpu.VMEM((nlon * pairs, PIECE), jnp.float32)],
        input_output_aliases=aliases,
        compiler_params=pltpu.CompilerParams(vmem_limit_bytes=32 << 20),
        cost_estimate=pl.CostEstimate(
            flops=2 * nlon * depth * group * PIECE * steps,
            bytes_accessed=6 * nlon * pairs * PIECE * steps,
            transcendentals=0,
        ),
        name="field_products",
    )(*args)


def per_device(coefficients, leaf_factors, level_interpolants, latitude_factors, order_ids):
    m, parts, fields, leaf = coefficients.shape
    size = lax.axis_size("ord")
    group = fields // size
    half = size // 2
    side = (lax.axis_index("ord") >> 1) & 1
    by_side = coefficients.reshape(m, parts, size // 4, 2, 2 * group, leaf)

    def leaves(which):
        chosen = lax.dynamic_index_in_dim(by_side, which, 3, keepdims=False)
        flat = chosen.reshape(m, parts * half * group, leaf)
        return jnp.einsum(
            "mcl,mrl->mcr", flat, leaf_factors, preferred_element_type=jnp.float32
        ).astype(jnp.bfloat16)

    top = lax.axis_size("blk") // 2

    def level(k, here, there):
        mixed = jnp.einsum(
            "mcx,mhx->mch", here, level_interpolants[k, 0], preferred_element_type=jnp.float32
        ) + jnp.einsum(
            "mcx,mhx->mch", there, level_interpolants[k, 1], preferred_element_type=jnp.float32
        )
        return mixed.astype(jnp.bfloat16)

    near, far = leaves(side), leaves(1 - side)
    crossing = lambda shard: xor_permute(shard, "ord", 2)
    pieces = [crossing(latitude_factors[:, begin:end]) for begin, end in zip(CUTS[:-1], CUTS[1:])]
    for k in range(level_interpolants.shape[0]):
        near = level(k, near, xor_permute(near, "blk", top >> k))
        far = level(k, far, xor_permute(far, "blk", top >> k))
    crossed = crossing(far)
    groups = [[i for i in range(size) if (i >> 1) & 1 == s] for s in (0, 1)]

    def regroup(reduced, factors):
        values = latitude_values(reduced, factors, parts)
        values = values.reshape((half, group) + values.shape[1:])
        return lax.all_to_all(values, "ord", 0, 0, axis_index_groups=groups, tiled=True)

    table = synthesis_table(order_ids, NLON, PERIOD).reshape(size // 4, 2, 2 * m * parts, NLON)

    def rows(which):
        return lax.dynamic_index_in_dim(table, which, 1, keepdims=False).reshape(half * m * parts, NLON)

    here, across = rows(side), rows(1 - side)
    near_values = regroup(near, [latitude_factors])
    first = regroup(crossed, pieces[:1])
    place = lax.axis_index("ord")
    column, core = place >> 2, place & 1
    quarter = size // 4
    shifts = [(2, 0), (2, 1), (1, 0), (3, 0), (1, 1), (3, 1), (0, 1), (0, 0)]
    to = jnp.stack([((column + a) % quarter) * 2 + (core ^ b) for a, b in shifts])
    source = jnp.stack([((column - a) % quarter) * 2 + (core ^ b) for a, b in shifts])
    to = to.astype(jnp.int32)
    later = []
    for factors in pieces[1:]:
        chunks = split_values(crossed, factors, parts, group, to)
        for k, (a, b) in enumerate(shifts):
            if (a, b) != (0, 0):
                pairs = [
                    (i, (((i >> 2) + a) % quarter) * 4 + (i & 2) + ((i & 1) ^ b))
                    for i in range(size)
                ]
                chunks[k] = lax.ppermute(chunks[k], "ord", pairs)
        later.append([chunk[None] for chunk in chunks])
    moved = jnp.take(
        across.reshape(half, m * parts, NLON), source, axis=0, mode="clip"
    ).reshape(across.shape)
    out = field_products(jnp.concatenate([here, across], 0).T, near_values, [first], 0, None)
    for i, chunks in enumerate(later):
        out = field_products(
            jnp.concatenate([here, moved], 0).T, near_values, chunks, CUTS[i + 1] // PIECE, out
        )
    return out


def solution(mesh):
    in_specs = (
        P("ord", None, None, "blk"),
        P("ord", None, "blk"),
        P(None, None, "ord", None, "blk"),
        P("ord", "blk", None),
        P(),
    )
    out_specs = P(None, "ord", "blk")

    return jax.shard_map(per_device, mesh=mesh, in_specs=in_specs, out_specs=out_specs, check_vma=False)
```

```python
import math

import jax
import jax.numpy as jnp
from jax import lax
from jax.experimental import pallas as pl
from jax.experimental.pallas import tpu as pltpu
from jax.sharding import PartitionSpec as P


PERIOD = 16384
NLON = 256
CUTS = (0, 384, 640)
PIECE = 128


def xor_permute(shard, axis, mask):
    return lax.ppermute(shard, axis, [(i, i ^ mask) for i in range(lax.axis_size(axis))])


def synthesis_table(order_ids, count, period):
    steps = jnp.arange(count, dtype=jnp.int32)
    phase = (order_ids[:, None] * steps[None, :] % period).astype(jnp.float32) * (
        2.0 * math.pi / period
    )
    weight = jnp.where(order_ids == 0, 1.0, 2.0).astype(jnp.float32)[:, None]
    table = jnp.stack([weight * jnp.cos(phase), -weight * jnp.sin(phase)], axis=1)
    return table.astype(jnp.bfloat16)


def latitude_values(reduced, factors, parts):
    m, count, rank = reduced.shape
    cols = count // parts
    lats = sum(f.shape[1] for f in factors)
    steps = lats // PIECE
    per = steps // len(factors)

    def body(reduced_ref, *refs):
        factor_refs, out_ref, wide = refs[: len(factors)], refs[-2], refs[-1]
        for j, factor_ref in enumerate(factor_refs):
            for i in range(per):
                for o in range(m):
                    acc = lax.dot_general(
                        reduced_ref[o],
                        factor_ref[o, i * PIECE : (i + 1) * PIECE],
                        (((1,), (1,)), ((), ())),
                        preferred_element_type=jnp.float32,
                    )
                    for p in range(parts):
                        wide[pl.ds(o * parts + p, cols, stride=m * parts), :] = acc[
                            p * cols : (p + 1) * cols
                        ]
                start = (j * per + i) * PIECE
                out_ref[:, :, start : start + PIECE] = (
                    wide[...].reshape(cols, m * parts, PIECE).astype(jnp.bfloat16)
                )

    flops = 2 * m * count * rank * lats
    return pl.pallas_call(
        body,
        out_shape=jax.ShapeDtypeStruct((cols, m * parts, lats), jnp.bfloat16),
        in_specs=[pl.BlockSpec(memory_space=pltpu.VMEM)] * (1 + len(factors)),
        out_specs=pl.BlockSpec(memory_space=pltpu.VMEM),
        scratch_shapes=[pltpu.VMEM((cols * m * parts, PIECE), jnp.float32)],
        compiler_params=pltpu.CompilerParams(vmem_limit_bytes=32 << 20),
        cost_estimate=pl.CostEstimate(flops=flops, bytes_accessed=2 * cols * m * parts * lats, transcendentals=0),
        name="latitude_values",
    )(reduced, *factors)


def split_values(reduced, factors, parts, group, order):
    m, count, rank = reduced.shape
    cols = count // parts
    dests = cols // group
    lats = factors.shape[1]
    mp = m * parts

    def body(order_ref, reduced_ref, factor_ref, *refs):
        outs, wide = refs[:-1], refs[-1]
        for start in range(0, lats, PIECE):
            for o in range(m):
                acc = lax.dot_general(
                    reduced_ref[o],
                    factor_ref[o, start : start + PIECE],
                    (((1,), (1,)), ((), ())),
                    preferred_element_type=jnp.float32,
                )
                for p in range(parts):
                    wide[pl.ds(o * parts + p, cols, stride=mp), :] = acc[p * cols : (p + 1) * cols]
            for k, out_ref in enumerate(outs):
                row = pl.multiple_of(order_ref[k] * (group * mp), group * mp)
                chosen = wide[pl.ds(row, group * mp), :]
                out_ref[:, :, start : start + PIECE] = chosen.reshape(group, mp, PIECE).astype(
                    jnp.bfloat16
                )

    return list(pl.pallas_call(
        body,
        out_shape=[jax.ShapeDtypeStruct((group, mp, lats), jnp.bfloat16)] * dests,
        in_specs=[pl.BlockSpec(memory_space=pltpu.SMEM)]
        + [pl.BlockSpec(memory_space=pltpu.VMEM)] * 2,
        out_specs=[pl.BlockSpec(memory_space=pltpu.VMEM)] * dests,
        scratch_shapes=[pltpu.VMEM((cols * mp, PIECE), jnp.float32)],
        compiler_params=pltpu.CompilerParams(vmem_limit_bytes=32 << 20),
        cost_estimate=pl.CostEstimate(
            flops=2 * m * count * rank * lats, bytes_accessed=2 * cols * mp * lats, transcendentals=0
        ),
        name="split_values",
    )(order, reduced, factors))


def field_products(table, near_values, far_values, first, out):
    half, group, mp, lats = near_values.shape
    nlon, depth = table.shape
    count = len(far_values)
    steps = far_values[0].shape[-1] // PIECE
    pairs = group // 2

    def body(table_ref, near_ref, *refs):
        far_refs, out_ref, wide = refs[:count], refs[-2], refs[-1]
        for p in range(pairs):
            sides = [
                jnp.concatenate(
                    [ref[:, f].reshape(-1, PIECE) for ref in (near_ref, *far_refs)], 0
                )
                for f in (2 * p, 2 * p + 1)
            ]
            grid = jnp.dot(
                table_ref[...], jnp.concatenate(sides, 1), preferred_element_type=jnp.float32
            )
            wide[pl.ds(p, nlon, stride=pairs), :] = grid[:, :PIECE] * grid[:, PIECE:]
        out_ref[...] = wide[...].reshape(nlon, pairs, PIECE).astype(jnp.bfloat16)

    block = (half, group, mp, PIECE)
    in_specs = [
        pl.BlockSpec((nlon, depth), lambda i: (0, 0)),
        pl.BlockSpec(block, lambda i: (0, 0, 0, first + i)),
    ]
    in_specs += [
        pl.BlockSpec((half // count, group, mp, PIECE), lambda i: (0, 0, 0, i)) for _ in range(count)
    ]
    args, aliases = [table, near_values, *far_values], {}
    if out is not None:
        in_specs.append(pl.BlockSpec(memory_space=pl.ANY))
        args.append(out)
        aliases = {2 + count: 0}
    return pl.pallas_call(
        body,
        grid=(steps,),
        out_shape=jax.ShapeDtypeStruct((nlon, pairs, lats), jnp.bfloat16),
        in_specs=in_specs,
        out_specs=pl.BlockSpec((nlon, pairs, PIECE), lambda i: (0, 0, first + i)),
        scratch_shapes=[pltpu.VMEM((nlon * pairs, PIECE), jnp.float32)],
        input_output_aliases=aliases,
        compiler_params=pltpu.CompilerParams(vmem_limit_bytes=32 << 20),
        cost_estimate=pl.CostEstimate(
            flops=2 * nlon * depth * group * PIECE * steps,
            bytes_accessed=6 * nlon * pairs * PIECE * steps,
            transcendentals=0,
        ),
        name="field_products",
    )(*args)


def per_device(coefficients, leaf_factors, level_interpolants, latitude_factors, order_ids):
    m, parts, fields, leaf = coefficients.shape
    size = lax.axis_size("ord")
    group = fields // size
    half = size // 2
    side = (lax.axis_index("ord") >> 1) & 1
    by_side = coefficients.reshape(m, parts, size // 4, 2, 2 * group, leaf)

    def leaves(which, source):
        chosen = lax.dynamic_index_in_dim(source, which, 3, keepdims=False)
        flat = chosen.reshape(m, parts * half * group, leaf)
        return jnp.einsum(
            "mcl,mrl->mcr", flat, leaf_factors, preferred_element_type=jnp.float32
        ).astype(jnp.bfloat16)

    top = lax.axis_size("blk") // 2

    def level(k, here, there):
        mixed = jnp.einsum(
            "mcx,mhx->mch", here, level_interpolants[k, 0], preferred_element_type=jnp.float32
        ) + jnp.einsum(
            "mcx,mhx->mch", there, level_interpolants[k, 1], preferred_element_type=jnp.float32
        )
        return mixed.astype(jnp.bfloat16)

    far = leaves(1 - side, by_side)
    near = leaves(side, lax.optimization_barrier((by_side, far))[0])
    crossing = lambda shard: xor_permute(shard, "ord", 2)
    pieces = [crossing(latitude_factors[:, begin:end]) for begin, end in zip(CUTS[:-1], CUTS[1:])]
    for k in range(level_interpolants.shape[0]):
        near = level(k, near, xor_permute(near, "blk", top >> k))
        far = level(k, far, xor_permute(far, "blk", top >> k))
    crossed = crossing(far)
    groups = [[i for i in range(size) if (i >> 1) & 1 == s] for s in (0, 1)]

    def regroup(reduced, factors):
        values = latitude_values(reduced, factors, parts)
        values = values.reshape((half, group) + values.shape[1:])
        return lax.all_to_all(values, "ord", 0, 0, axis_index_groups=groups, tiled=True)

    table = synthesis_table(order_ids, NLON, PERIOD).reshape(size // 4, 2, 2 * m * parts, NLON)

    def rows(which):
        return lax.dynamic_index_in_dim(table, which, 1, keepdims=False).reshape(half * m * parts, NLON)

    here, across = rows(side), rows(1 - side)
    near_values = regroup(near, [latitude_factors])
    first = regroup(crossed, pieces[:1])
    place = lax.axis_index("ord")
    column, core = place >> 2, place & 1
    quarter = size // 4
    shifts = [(2, 0), (2, 1), (1, 0), (3, 0), (1, 1), (3, 1), (0, 1), (0, 0)]
    to = jnp.stack([((column + a) % quarter) * 2 + (core ^ b) for a, b in shifts])
    source = jnp.stack([((column - a) % quarter) * 2 + (core ^ b) for a, b in shifts])
    to = to.astype(jnp.int32)
    later = []
    for factors in pieces[1:]:
        chunks = split_values(crossed, factors, parts, group, to)
        for k, (a, b) in enumerate(shifts):
            if (a, b) != (0, 0):
                pairs = [
                    (i, (((i >> 2) + a) % quarter) * 4 + (i & 2) + ((i & 1) ^ b))
                    for i in range(size)
                ]
                chunks[k] = lax.ppermute(chunks[k], "ord", pairs)
        later.append([chunk[None] for chunk in chunks])
    moved = jnp.take(
        across.reshape(half, m * parts, NLON), source, axis=0, mode="clip"
    ).reshape(across.shape)
    out = field_products(jnp.concatenate([here, across], 0).T, near_values, [first], 0, None)
    for i, chunks in enumerate(later):
        out = field_products(
            jnp.concatenate([here, moved], 0).T, near_values, chunks, CUTS[i + 1] // PIECE, out
        )
    return out


def solution(mesh):
    in_specs = (
        P("ord", None, None, "blk"),
        P("ord", None, "blk"),
        P(None, None, "ord", None, "blk"),
        P("ord", "blk", None),
        P(),
    )
    out_specs = P(None, "ord", "blk")

    return jax.shard_map(per_device, mesh=mesh, in_specs=in_specs, out_specs=out_specs, check_vma=False)
```
